32 devices in a mesh: dp: 16 (over z, y, x), sub: 2 (over core).
Axes of the slice: x: 2, y: 2, z: 4, core: 2. Of those that a mesh axis runs over, the one named last changes fastest.
Arguments:
- projections: float32 [6144, 128], P(('dp', 'sub')), may hold values from -6 to 6
- partner: int32 [6144], P(('dp', 'sub')), may hold values from 0 to 6143, as said below
Outputs:
- loss: float32 [], replicated
- grad_projections: float32 [6144, 128], P(('dp', 'sub'))
The draws below stay inside these ranges and needn't reach their ends.
Inputs may be any that keep to these rules, and one draw needn't show every extreme that they name: partner pairs the views: partner[partner[i]] = i and partner[i] != i for every view.
All inputs are finite; a program needn't handle non-finite values.
Results may differ from the reference program's by a relative error of at most 0.0003.
The reference program's roundings to bfloat16 on the way (of `unit_low` and `weight`) count: a program that leaves them out, or rounds other values in their place, can miss the bound.
Values may be sent and summed in bfloat16 or wider, within the bound.
A program may use at most 128 MiB of HBM per device.

```python
import jax
import jax.numpy as jnp
from jax import lax

D = 128
V_DEV = 192
VIEWS = 6144
N_SUB = 2


def draw_partner(key, part):
    order = jax.random.permutation(key, VIEWS).astype(jnp.int32)
    pairs = order.reshape(VIEWS // 2, 2)
    result = jnp.zeros((VIEWS,), jnp.int32)
    result = result.at[pairs[:, 0]].set(pairs[:, 1])
    result = result.at[pairs[:, 1]].set(pairs[:, 0])
    return result


def steps_of(own_key, dims, split, low, largest):
    factor_of = 1.0
    for axis_at, blocks in split:
        steps = jax.random.uniform(jax.random.fold_in(jax.random.fold_in(own_key, 6), axis_at), (blocks,), jnp.float32, low / len(split), largest / len(split))
        factor_of = factor_of * jnp.repeat(jnp.exp(steps), dims[axis_at] // blocks).reshape((-1,) + (1,) * (len(dims) - 1 - axis_at))
    return factor_of


def scatter_about(rng, extent, scale, limit, pieces=(), kind=jnp.bfloat16):
    entries = scale * jax.random.normal(rng, extent, jnp.float32)
    if pieces:
        entries = entries * steps_of(rng, extent, pieces, -0.22, 0.18)
    return jnp.clip(entries, -limit, limit).astype(kind)


def setup_inputs(seed: int = 0) -> dict:
    streams_of = jax.random.split(jax.random.key(seed), 3)
    projections = scatter_about(streams_of[0], (VIEWS, D), 1.0, 6.0, ((0, 32),), jnp.float32)
    partner = draw_partner(jax.random.fold_in(streams_of[2], 71), 0)
    return {"projections": projections, "partner": partner}


TAU = 0.1
SHIFT = 10.0

def reference(projections, partner):
    inverse = lax.rsqrt(lax.optimization_barrier(jnp.sum(projections * projections, axis=1)) + 1e-06)
    unit = projections * inverse[:, None]
    unit_low = unit.astype(jnp.bfloat16)
    block = V_DEV * N_SUB
    count = VIEWS // block
    columns = jnp.arange(VIEWS, dtype=jnp.int32)

    def scores_of(index):
        start = (index * block).astype(jnp.int32)
        rows_low = lax.dynamic_slice_in_dim(unit_low, start, block, 0)
        score = jnp.dot(rows_low, unit_low.T, preferred_element_type=jnp.float32) / TAU
        rows = start + jnp.arange(block, dtype=jnp.int32)
        diag = columns[None, :] == rows[:, None]
        mates = lax.dynamic_slice_in_dim(partner, start, block, 0)
        hit = columns[None, :] == mates[:, None]
        return (score, diag, hit)

    def forward(index):
        score, diag, hit = scores_of(index)
        total = lax.optimization_barrier(jnp.sum(jnp.where(diag, 0.0, jnp.exp(score - SHIFT)), axis=1))
        lse = jnp.log(total) + SHIFT
        pos = lax.optimization_barrier(jnp.sum(jnp.where(hit, score, 0.0), axis=1))
        return (lse, lse - pos)
    lse, row_loss = lax.map(forward, jnp.arange(count, dtype=jnp.int32))
    lse = lse.reshape(VIEWS)
    row_loss = row_loss.reshape(VIEWS)
    loss = jnp.sum(row_loss) / VIEWS

    def backward(index):
        score, diag, hit = scores_of(index)
        start = (index * block).astype(jnp.int32)
        lse_rows = lax.dynamic_slice_in_dim(lse, start, block, 0)
        weight = jnp.exp(score - lse_rows[:, None]) + jnp.exp(score - lse[None, :])
        weight = weight - 2.0 * hit.astype(jnp.float32)
        weight = jnp.where(diag, 0.0, weight / TAU).astype(jnp.bfloat16)
        return jnp.dot(weight, unit_low, preferred_element_type=jnp.float32)
    grad_unit = lax.map(backward, jnp.arange(count, dtype=jnp.int32)).reshape(VIEWS, D)
    inner = lax.optimization_barrier(jnp.sum(unit * grad_unit, axis=1))
    grad = inverse[:, None] * (grad_unit - unit * inner[:, None])
    return (loss, grad)
```

```python
import functools
import math

import jax
import jax.numpy as jnp
from jax import lax
from jax.experimental import pallas as pl
from jax.experimental.pallas import tpu as pltpu
from jax.sharding import PartitionSpec as P

TAU = 0.1
SHIFT = 10.0
EPS = 1e-06
LANES = 128
MESH = pl.DeviceIdType.MESH
LINE = 4

FORWARD = (
    (0, 0, 0), (0, 0, 1), (1, 0, 0), (1, 0, 1), (0, 1, 0), (0, 1, 1), (2, 0, 0), (2, 0, 1),
    (1, 1, 0), (1, 1, 1), (3, 0, 0), (3, 0, 1), (2, 1, 0), (2, 1, 1), (3, 1, 0), (3, 1, 1),
)


def plan():
    at = {step: i for i, step in enumerate(FORWARD)}
    chunks = []
    for place in range(LINE):
        for dx in range(2):
            for dy in range(2):
                chunks.append((max(at[(place, dy, dx)], at[(place, dx, dy)]), (place, dx, dy)))
    chunks.sort()
    out = []
    for i, step in enumerate(FORWARD):
        out.append(("step", step))
        if chunks and chunks[0][0] < i:
            out.append(("chunk", chunks.pop(0)[1]))
    out.extend(("chunk", c) for _, c in chunks)
    return out


def kernel(
    groups, p_ref, partner_ref, loss_ref, grad_ref,
    blocks, scores, totals, accum, pos, gsum, unit_s, mates, send, recv, rsend, rrecv,
):
    rows = p_ref.shape[0]
    pair = 2 * rows
    tiles = pair // LANES
    spare = 2 * LANES - rows
    d = lax.axis_index("dp")
    c = lax.axis_index("sub")
    z = d // 4
    y = (d // 2) % 2
    x = d % 2
    me = d * 2 + c
    first = x * (1 - c) + y * c
    last = y * (1 - c) + x * c
    half = z // 2

    def place_z(k):
        return (z, z + 1 - 2 * (z % 2), 2 - half, 3 - 3 * half)[k]

    def chip_of(zz, f, l):
        return zz * 4 + f * (1 + c) + l * (2 - c)

    flip = lambda v, n: v + n * (1 - 2 * v)
    near_first = (chip_of(z, flip(first, 1), last), c)
    near_last = (chip_of(z, first, flip(last, 1)), c)
    sibling = (d, 1 - c)
    up, down = (d + 4, c), (d - 4, c)

    barrier = pltpu.get_barrier_semaphore()
    for dev in (near_first, near_last, sibling):
        pl.semaphore_signal(barrier, inc=1, device_id=dev, device_id_type=MESH)

    @pl.when(z < LINE - 1)
    def _():
        pl.semaphore_signal(barrier, inc=1, device_id=up, device_id_type=MESH)

    @pl.when(z > 0)
    def _():
        pl.semaphore_signal(barrier, inc=1, device_id=down, device_id_type=MESH)

    p = p_ref[...]
    inverse = lax.rsqrt(jnp.sum(p * p, axis=1, keepdims=True) + EPS)
    unit = p * inverse
    own = unit.astype(jnp.bfloat16)
    blocks[me] = own
    unit_s[...] = unit
    accum[...] = jnp.zeros_like(accum)
    pos[...] = jnp.zeros_like(pos)
    gsum[...] = jnp.zeros_like(gsum)
    spread = jnp.broadcast_to(partner_ref[...].astype(jnp.float32), (LANES, rows)).T
    mates[...] = spread.astype(jnp.int32) - lax.broadcasted_iota(jnp.int32, (rows, LANES), 1)
    mine = pl.ds(pl.multiple_of(c * spare, 8), rows)

    pl.semaphore_wait(barrier, 3 + jnp.minimum(z, 1) + jnp.minimum(LINE - 1 - z, 1))

    def copy(b, dev, i, way):
        return pltpu.make_async_remote_copy(
            src_ref=blocks.at[b],
            dst_ref=blocks.at[b],
            send_sem=send.at[i, way],
            recv_sem=recv.at[b],
            device_id=dev,
            device_id_type=MESH,
        )

    def sends(step, act):
        k, dl, df = step
        i = FORWARD.index(step)
        zz = place_z(k)
        b = chip_of(zz, flip(first, df), flip(last, dl)) * 2 + c
        if dl == 0:
            if k == 0:
                go_up, go_down = z < LINE - 1, z > 0
            else:
                go_up = jnp.logical_and(zz < z, z < LINE - 1)
                go_down = jnp.logical_and(zz > z, z > 0)

            @pl.when(go_up)
            def _():
                act(copy(b, up, i, 0))

            @pl.when(go_down)
            def _():
                act(copy(b, down, i, 1))

            if k == 0 and df == 0:
                act(copy(b, near_first, i, 4))
            act(copy(b, near_last, i, 2))
        act(copy(b, sibling, i, 3))
        return b

    def forward(step):
        k, dl, df = step
        if (k, dl, df) != (0, 0, 0):
            b = chip_of(place_z(k), flip(first, df), flip(last, dl)) * 2 + c
            copy(b, sibling, 0, 0).wait_recv()
        sends(step, lambda one: one.start())

    def chip_at(chunk):
        k, dx, dy = chunk
        return place_z(k) * 4 + flip(y, dy) * 2 + flip(x, dx)

    def pair_of(chip):
        return blocks[pl.ds(2 * chip, 2)].reshape(pair, LANES)

    scale = math.log2(math.e) / TAU

    def chunk_forward(n, chunk):
        chip = chip_at(chunk)
        copy(chip * 2 + 1 - c, sibling, 0, 0).wait_recv()
        dots = lax.dot_general(
            blocks[me], pair_of(chip), (((1,), (1,)), ((), ())), preferred_element_type=jnp.float32
        )
        powers = jnp.exp2(dots * scale - SHIFT * math.log2(math.e))
        if chunk == (0, 0, 0):
            cols = lax.broadcasted_iota(jnp.int32, (rows, pair), 1)
            at = lax.broadcasted_iota(jnp.int32, (rows, pair), 0) + c * rows
            powers = jnp.where(cols == at, 0.0, powers)
        scores[n] = powers
        total = accum[mine, :]
        found = pos[...]
        for t in range(tiles):
            part = slice(t * LANES, (t + 1) * LANES)
            total = total + powers[:, part]
            hit = mates[...] == chip * pair + t * LANES
            found = found + jnp.where(hit, dots[:, part], 0.0)
        accum[mine, :] = total
        pos[...] = found

    order = []
    for what, item in plan():
        if what == "step":
            forward(item)
        else:
            chunk_forward(len(order), item)
            order.append(item)

    every = accum[...]
    totals[me, :, 0 : 2 * LANES] = jnp.sum(every.T, axis=0, keepdims=True)
    totals[me, :, 2 * LANES : 3 * LANES] = jnp.sum(pos[...], axis=0, keepdims=True) / TAU

    def share(j):
        to = lax.rem(me + j, groups)
        return pltpu.make_async_remote_copy(
            src_ref=totals.at[me],
            dst_ref=totals.at[me],
            send_sem=rsend.at[j],
            recv_sem=rrecv.at[me],
            device_id=(to // 2, to % 2),
            device_id_type=MESH,
        )

    def shared(b):
        return pltpu.make_async_remote_copy(
            src_ref=totals.at[b],
            dst_ref=totals.at[b],
            send_sem=rsend.at[0],
            recv_sem=rrecv.at[b],
            device_id=sibling,
            device_id_type=MESH,
        )

    @pl.loop(1, groups)
    def _(j):
        share(j).start()

    row_scale = (1.0 / TAU) / jnp.sum(accum[mine, :], axis=1, keepdims=True)
    low = lax.broadcasted_iota(jnp.int32, (1, LANES), 1) < rows - LANES

    def columns(chip):
        a, b = totals[2 * chip], totals[2 * chip + 1]
        return (
            a[:, :LANES],
            jnp.where(low, a[:, LANES : 2 * LANES], b[:, :LANES]),
            b[:, LANES : 2 * LANES],
        )

    for n, chunk in enumerate(order):
        chip = chip_at(chunk)
        shared(2 * chip + 1 - c).wait_recv()
        if chunk != (0, 0, 0):
            shared(2 * chip + c).wait_recv()
        powers = scores[n]
        parts = []
        for t, column in enumerate(columns(chip)):
            weight = powers[:, t * LANES : (t + 1) * LANES] * (row_scale + (1.0 / TAU) / column)
            hit = mates[...] == chip * pair + t * LANES
            parts.append(jnp.where(hit, weight - 2.0 / TAU, weight).astype(jnp.bfloat16))
        gsum[...] += jnp.dot(
            jnp.concatenate(parts, axis=1), pair_of(chip), preferred_element_type=jnp.float32
        )

    grown = gsum[...]
    unit = unit_s[...]
    p = p_ref[...]
    inverse = lax.rsqrt(jnp.sum(p * p, axis=1, keepdims=True) + EPS)
    inner = jnp.sum(unit * grown, axis=1, keepdims=True)
    grad_ref[...] = inverse * (grown - unit * inner)

    logs = jnp.zeros((1, LANES), jnp.float32)
    for chip in range(groups // 2):
        for column in columns(chip):
            logs = logs + jnp.log(column)
        for core in range(2):
            logs = logs - totals[2 * chip + core][:, 2 * LANES : 3 * LANES]
    loss_ref[0, 0] = jnp.sum(logs) / (rows * groups) + SHIFT

    for step in FORWARD:
        sends(step, lambda one: one.wait_send())

    @pl.loop(1, groups)
    def _(j):
        share(j).wait_send()


def fused(projections, partner):
    rows, width = projections.shape
    groups = lax.axis_size(("dp", "sub"))
    chips = groups // 2
    loss, grad = pl.pallas_call(
        functools.partial(kernel, groups),
        out_shape=(
            jax.ShapeDtypeStruct((1, 1), jnp.float32),
            jax.ShapeDtypeStruct((rows, width), jnp.float32),
        ),
        in_specs=[pl.BlockSpec(memory_space=pltpu.VMEM)] * 2,
        out_specs=(
            pl.BlockSpec(memory_space=pltpu.SMEM),
            pl.BlockSpec(memory_space=pltpu.VMEM),
        ),
        scratch_shapes=[
            pltpu.VMEM((groups, rows, width), jnp.bfloat16),
            pltpu.VMEM((chips, rows, 2 * rows), jnp.float32),
            pltpu.VMEM((groups, 1, 3 * LANES), jnp.float32),
            pltpu.VMEM((2 * LANES, LANES), jnp.float32),
            pltpu.VMEM((rows, LANES), jnp.float32),
            pltpu.VMEM((rows, width), jnp.float32),
            pltpu.VMEM((rows, width), jnp.float32),
            pltpu.VMEM((rows, LANES), jnp.int32),
            pltpu.SemaphoreType.DMA((len(FORWARD), 5)),
            pltpu.SemaphoreType.DMA((groups,)),
            pltpu.SemaphoreType.DMA((groups,)),
            pltpu.SemaphoreType.DMA((groups,)),
        ],
        compiler_params=pltpu.CompilerParams(collective_id=0, has_side_effects=True),
    )(projections, partner.reshape(1, rows))
    return loss.reshape(()), grad


def general(projections, partner):
    rows = projections.shape[0]
    axes = ("dp", "sub")
    inverse = lax.rsqrt(jnp.sum(projections * projections, axis=1) + EPS)
    unit = projections * inverse[:, None]
    low = unit.astype(jnp.bfloat16)
    everyone = lax.all_gather(low, axes, axis=0, tiled=True)
    columns = jnp.arange(everyone.shape[0], dtype=jnp.int32)
    ids = lax.axis_index(axes) * rows + jnp.arange(rows, dtype=jnp.int32)
    score = (
        lax.dot_general(
            low, everyone, (((1,), (1,)), ((), ())), preferred_element_type=jnp.float32
        )
        / TAU
    )
    diag = columns[None, :] == ids[:, None]
    hit = columns[None, :] == partner[:, None]
    total = jnp.sum(jnp.where(diag, 0.0, jnp.exp(score - SHIFT)), axis=1)
    found = jnp.sum(jnp.where(hit, score, 0.0), axis=1)
    lse = jnp.log(total) + SHIFT
    lse_all = lax.all_gather(lse, axes, axis=0, tiled=True)
    loss = lax.psum(jnp.sum(lse - found), axes) / everyone.shape[0]
    weight = jnp.exp(score - lse[:, None]) + jnp.exp(score - lse_all[None, :])
    weight = weight - 2.0 * hit.astype(jnp.float32)
    weight = jnp.where(diag, 0.0, weight / TAU).astype(jnp.bfloat16)
    grown = jnp.dot(weight, everyone, preferred_element_type=jnp.float32)
    inner = jnp.sum(unit * grown, axis=1)
    return loss, inverse[:, None] * (grown - unit * inner[:, None])


def solution(mesh):
    small = mesh.shape["dp"] == 4 * LINE and mesh.shape["sub"] == 2

    def body(projections, partner):
        rows, width = projections.shape
        fits = width == LANES and LANES < rows < 2 * LANES and (2 * rows) % LANES == 0
        return (fused if small and fits else general)(projections, partner)

    return jax.shard_map(
        body,
        mesh=mesh,
        in_specs=(P(("dp", "sub"), None), P(("dp", "sub"))),
        out_specs=(P(), P(("dp", "sub"), None)),
        check_vma=False,
    )
```

```python
import functools
import math

import jax
import jax.numpy as jnp
from jax import lax
from jax.experimental import pallas as pl
from jax.experimental.pallas import tpu as pltpu
from jax.sharding import PartitionSpec as P

TAU = 0.1
SHIFT = 10.0
EPS = 1e-06
LANES = 128
MESH = pl.DeviceIdType.MESH
LINE = 4

FORWARD = (
    (0, 0, 0), (1, 0, 0), (2, 0, 0), (3, 0, 0), (0, 0, 1), (0, 1, 0), (0, 1, 1), (1, 0, 1),
    (1, 1, 0), (1, 1, 1), (2, 0, 1), (2, 1, 0), (2, 1, 1), (3, 0, 1), (3, 1, 0), (3, 1, 1),
)
EARLY = 4
WAYS = 7


def plan():
    at = {step: i for i, step in enumerate(FORWARD)}
    chunks = []
    for place in range(LINE):
        for dx in range(2):
            for dy in range(2):
                chunks.append((max(at[(place, dy, dx)], at[(place, dx, dy)]), (place, dx, dy)))
    chunks.sort()
    out = []
    for i, step in enumerate(FORWARD):
        out.append(("step", step))
        if i >= EARLY and chunks and chunks[0][0] < i:
            out.append(("chunk", chunks.pop(0)[1]))
    out.extend(("chunk", c) for _, c in chunks)
    return out


def kernel(
    groups, p_hbm, partner_hbm, loss_ref, grad_ref, p_ref, partner_ref,
    blocks, scores, totals, accum, pos, gsum, unit_s, mates, fetched, send, recv, rsend, rrecv,
):
    rows = p_hbm.shape[0]
    pair = 2 * rows
    tiles = pair // LANES
    spare = 2 * LANES - rows
    d = lax.axis_index("dp")
    c = lax.axis_index("sub")
    z = d // 4
    y = (d // 2) % 2
    x = d % 2
    me = d * 2 + c
    first = x * (1 - c) + y * c
    last = y * (1 - c) + x * c
    half = z // 2

    def place_z(k):
        return (z, z + 1 - 2 * (z % 2), 2 - half, 3 - 3 * half)[k]

    def chip_of(zz, f, l):
        return zz * 4 + f * (1 + c) + l * (2 - c)

    flip = lambda v, n: v + n * (1 - 2 * v)
    near_first = (chip_of(z, flip(first, 1), last), c)
    near_last = (chip_of(z, first, flip(last, 1)), c)
    diagonal = (chip_of(z, flip(first, 1), flip(last, 1)), c)
    sibling = (d, 1 - c)
    line = [(chip_of(place_z(k), first, last), c) for k in (1, 2, 3)]

    fetch = pltpu.make_async_copy(p_hbm, p_ref, fetched.at[0])
    fetch.start()
    fetch_mates = pltpu.make_async_copy(partner_hbm, partner_ref, fetched.at[1])
    fetch_mates.start()
    barrier = pltpu.get_barrier_semaphore()
    peers = (*line, near_first, near_last, diagonal, sibling)
    for dev in peers:
        pl.semaphore_signal(barrier, inc=1, device_id=dev, device_id_type=MESH)

    accum[...] = jnp.zeros_like(accum)
    pos[...] = jnp.zeros_like(pos)
    gsum[...] = jnp.zeros_like(gsum)
    mine = pl.ds(pl.multiple_of(c * spare, 8), rows)
    fetch.wait()
    p = p_ref[...]
    inverse = lax.rsqrt(jnp.sum(p * p, axis=1, keepdims=True) + EPS)
    unit = p * inverse
    blocks[me] = unit.astype(jnp.bfloat16)
    unit_s[...] = unit
    fetch_mates.wait()
    spread = jnp.broadcast_to(partner_ref[...].astype(jnp.float32), (LANES, rows)).T
    mates[...] = spread.astype(jnp.int32) - lax.broadcasted_iota(jnp.int32, (rows, LANES), 1)

    pl.semaphore_wait(barrier, len(peers))

    def copy(b, dev, i, way):
        return pltpu.make_async_remote_copy(
            src_ref=blocks.at[b],
            dst_ref=blocks.at[b],
            send_sem=send.at[i, way],
            recv_sem=recv.at[b],
            device_id=dev,
            device_id_type=MESH,
        )

    def sends(step, act):
        k, dl, df = step
        i = FORWARD.index(step)
        zz = place_z(k)
        b = chip_of(zz, flip(first, df), flip(last, dl)) * 2 + c
        if (dl, df) == (0, 0):
            if k == 0:
                for way, dev in enumerate(line):
                    act(copy(b, dev, i, way))
            act(copy(b, diagonal, i, 5))
            act(copy(b, near_first, i, 3))
            act(copy(b, near_last, i, 4))
        act(copy(b, sibling, i, 6))
        return b

    def forward(step):
        k, dl, df = step
        if (k, dl, df) != (0, 0, 0):
            b = chip_of(place_z(k), flip(first, df), flip(last, dl)) * 2 + c
            copy(b, sibling, 0, 0).wait_recv()
        sends(step, lambda one: one.start())

    def chip_at(chunk):
        k, dx, dy = chunk
        return place_z(k) * 4 + flip(y, dy) * 2 + flip(x, dx)

    def pair_of(chip):
        return blocks[pl.ds(2 * chip, 2)].reshape(pair, LANES)

    scale = math.log2(math.e) / TAU

    def chunk_forward(n, chunk):
        chip = chip_at(chunk)
        copy(chip * 2 + 1 - c, sibling, 0, 0).wait_recv()
        dots = lax.dot_general(
            blocks[me], pair_of(chip), (((1,), (1,)), ((), ())), preferred_element_type=jnp.float32
        )
        powers = jnp.exp2(dots * scale - SHIFT * math.log2(math.e))
        if chunk == (0, 0, 0):
            cols = lax.broadcasted_iota(jnp.int32, (rows, pair), 1)
            at = lax.broadcasted_iota(jnp.int32, (rows, pair), 0) + c * rows
            powers = jnp.where(cols == at, 0.0, powers)
        scores[n] = powers
        total = accum[mine, :]
        found = pos[...]
        for t in range(tiles):
            part = slice(t * LANES, (t + 1) * LANES)
            total = total + powers[:, part]
            hit = mates[...] == chip * pair + t * LANES
            found = found + jnp.where(hit, dots[:, part], 0.0)
        accum[mine, :] = total
        pos[...] = found

    order = []
    for what, item in plan():
        if what == "step":
            forward(item)
        else:
            chunk_forward(len(order), item)
            order.append(item)

    every = accum[...]
    totals[me, :, 0 : 2 * LANES] = jnp.sum(every.T, axis=0, keepdims=True)
    totals[me, :, 2 * LANES : 3 * LANES] = jnp.sum(pos[...], axis=0, keepdims=True) / TAU

    def share(j):
        to = lax.rem(me + j, groups)
        return pltpu.make_async_remote_copy(
            src_ref=totals.at[me],
            dst_ref=totals.at[me],
            send_sem=rsend.at[j],
            recv_sem=rrecv.at[me],
            device_id=(to // 2, to % 2),
            device_id_type=MESH,
        )

    def shared(b):
        return pltpu.make_async_remote_copy(
            src_ref=totals.at[b],
            dst_ref=totals.at[b],
            send_sem=rsend.at[0],
            recv_sem=rrecv.at[b],
            device_id=sibling,
            device_id_type=MESH,
        )

    @pl.loop(1, groups)
    def _(j):
        share(j).start()

    row_scale = (1.0 / TAU) / jnp.sum(accum[mine, :], axis=1, keepdims=True)
    low = lax.broadcasted_iota(jnp.int32, (1, LANES), 1) < rows - LANES

    def columns(chip):
        a, b = totals[2 * chip], totals[2 * chip + 1]
        return (
            a[:, :LANES],
            jnp.where(low, a[:, LANES : 2 * LANES], b[:, :LANES]),
            b[:, LANES : 2 * LANES],
        )

    for n, chunk in enumerate(order):
        chip = chip_at(chunk)
        shared(2 * chip + 1 - c).wait_recv()
        if chunk != (0, 0, 0):
            shared(2 * chip + c).wait_recv()
        powers = scores[n]
        parts = []
        for t, column in enumerate(columns(chip)):
            weight = powers[:, t * LANES : (t + 1) * LANES] * (row_scale + (1.0 / TAU) / column)
            hit = mates[...] == chip * pair + t * LANES
            parts.append(jnp.where(hit, weight - 2.0 / TAU, weight).astype(jnp.bfloat16))
        gsum[...] += jnp.dot(
            jnp.concatenate(parts, axis=1), pair_of(chip), preferred_element_type=jnp.float32
        )

    grown = gsum[...]
    unit = unit_s[...]
    p = p_ref[...]
    inverse = lax.rsqrt(jnp.sum(p * p, axis=1, keepdims=True) + EPS)
    inner = jnp.sum(unit * grown, axis=1, keepdims=True)
    grad_ref[...] = inverse * (grown - unit * inner)

    logs = jnp.zeros((1, LANES), jnp.float32)
    for chip in range(groups // 2):
        for column in columns(chip):
            logs = logs + jnp.log(column)
        for core in range(2):
            logs = logs - totals[2 * chip + core][:, 2 * LANES : 3 * LANES]
    loss_ref[0, 0] = jnp.sum(logs) / (rows * groups) + SHIFT

    for step in FORWARD:
        sends(step, lambda one: one.wait_send())

    @pl.loop(1, groups)
    def _(j):
        share(j).wait_send()


def fused(projections, partner):
    rows, width = projections.shape
    groups = lax.axis_size(("dp", "sub"))
    chips = groups // 2
    loss, grad = pl.pallas_call(
        functools.partial(kernel, groups),
        out_shape=(
            jax.ShapeDtypeStruct((1, 1), jnp.float32),
            jax.ShapeDtypeStruct((rows, width), jnp.float32),
        ),
        in_specs=[pl.BlockSpec(memory_space=pl.ANY)] * 2,
        out_specs=(
            pl.BlockSpec(memory_space=pltpu.SMEM),
            pl.BlockSpec(memory_space=pltpu.VMEM),
        ),
        scratch_shapes=[
            pltpu.VMEM((rows, width), jnp.float32),
            pltpu.VMEM((1, rows), jnp.int32),
            pltpu.VMEM((groups, rows, width), jnp.bfloat16),
            pltpu.VMEM((chips, rows, 2 * rows), jnp.float32),
            pltpu.VMEM((groups, 1, 3 * LANES), jnp.float32),
            pltpu.VMEM((2 * LANES, LANES), jnp.float32),
            pltpu.VMEM((rows, LANES), jnp.float32),
            pltpu.VMEM((rows, width), jnp.float32),
            pltpu.VMEM((rows, width), jnp.float32),
            pltpu.VMEM((rows, LANES), jnp.int32),
            pltpu.SemaphoreType.DMA((2,)),
            pltpu.SemaphoreType.DMA((len(FORWARD), WAYS)),
            pltpu.SemaphoreType.DMA((groups,)),
            pltpu.SemaphoreType.DMA((groups,)),
            pltpu.SemaphoreType.DMA((groups,)),
        ],
        compiler_params=pltpu.CompilerParams(collective_id=0, has_side_effects=True),
    )(projections, partner.reshape(1, rows))
    return loss.reshape(()), grad


def general(projections, partner):
    rows = projections.shape[0]
    axes = ("dp", "sub")
    inverse = lax.rsqrt(jnp.sum(projections * projections, axis=1) + EPS)
    unit = projections * inverse[:, None]
    low = unit.astype(jnp.bfloat16)
    everyone = lax.all_gather(low, axes, axis=0, tiled=True)
    columns = jnp.arange(everyone.shape[0], dtype=jnp.int32)
    ids = lax.axis_index(axes) * rows + jnp.arange(rows, dtype=jnp.int32)
    score = (
        lax.dot_general(
            low, everyone, (((1,), (1,)), ((), ())), preferred_element_type=jnp.float32
        )
        / TAU
    )
    diag = columns[None, :] == ids[:, None]
    hit = columns[None, :] == partner[:, None]
    total = jnp.sum(jnp.where(diag, 0.0, jnp.exp(score - SHIFT)), axis=1)
    found = jnp.sum(jnp.where(hit, score, 0.0), axis=1)
    lse = jnp.log(total) + SHIFT
    lse_all = lax.all_gather(lse, axes, axis=0, tiled=True)
    loss = lax.psum(jnp.sum(lse - found), axes) / everyone.shape[0]
    weight = jnp.exp(score - lse[:, None]) + jnp.exp(score - lse_all[None, :])
    weight = weight - 2.0 * hit.astype(jnp.float32)
    weight = jnp.where(diag, 0.0, weight / TAU).astype(jnp.bfloat16)
    grown = jnp.dot(weight, everyone, preferred_element_type=jnp.float32)
    inner = jnp.sum(unit * grown, axis=1)
    return loss, inverse[:, None] * (grown - unit * inner[:, None])


def solution(mesh):
    small = mesh.shape["dp"] == 4 * LINE and mesh.shape["sub"] == 2

    def body(projections, partner):
        rows, width = projections.shape
        fits = width == LANES and LANES < rows < 2 * LANES and (2 * rows) % LANES == 0
        return (fused if small and fits else general)(projections, partner)

    return jax.shard_map(
        body,
        mesh=mesh,
        in_specs=(P(("dp", "sub"), None), P(("dp", "sub"))),
        out_specs=(P(), P(("dp", "sub"), None)),
        check_vma=False,
    )
```
